256 devices in a mesh: grp: 4 (over x_lo, core), seq: 64 (over y, x_hi, z).
Axes of the slice: x: 4 (x_hi: 2, x_lo: 2; x = x_hi * 2 + x_lo), y: 4, z: 8, core: 2. Of those that a mesh axis runs over, the one named last changes fastest.
Arguments:
- signal: bfloat16 [4, 8192, 2048], P('grp', 'seq'), may hold values from -6 to 6
- gate_in: bfloat16 [4, 8192, 2048], P('grp', 'seq'), may hold values from -6 to 6
- gate_out: bfloat16 [4, 8192, 2048], P('grp', 'seq'), may hold values from -6 to 6
- pos_weight: float32 [33, 64], replicated, may hold values from -1 to 1
- pos_bias: float32 [64], replicated, may hold values from -1 to 1
- inner_weight: float32 [2, 64, 64], replicated, may hold values from -0.75 to 0.75
- inner_bias: float32 [2, 64], replicated, may hold values from -1 to 1
- frequency: float32 [64], replicated, may hold values from 1 to 12
- out_weight: float32 [64, 2048], replicated, may hold values from -0.75 to 0.75
- decay_rates: float32 [2048], replicated, may hold values from 0.3 to 3000
- skip_gain: float32 [2048], replicated, may hold values from -6 to 6
Outputs:
- layer_out: bfloat16 [4, 8192, 2048], P('grp', 'seq')
The draws below stay inside these ranges and needn't reach their ends.
All inputs are finite; a program needn't handle non-finite values.
Results may differ from the reference program's by a relative error of at most 0.009.
Values may be sent and summed in bfloat16 or wider, within the bound.
No kernel may reach another device: no remote copies, remote signals or barrier semaphores. Data moves between devices by JAX's collectives and lax.ppermute only.
A program may use at most 64 MiB of HBM per device.

```python
import math
import jax
import jax.numpy as jnp
from jax import lax

D = 2048
ORDER = 64
EMB = 33
INNER = 2
POS_DEV = 128
SEQS = 4
SEQ = 8192
N_SEQ = 64


def level_of(own_key, shape, cuts, smallest, largest):
    def one(position, blocks):
        heights = jax.random.uniform(jax.random.fold_in(jax.random.fold_in(own_key, 6), position), (blocks,), jnp.float32, smallest / len(cuts), largest / len(cuts))
        return jnp.repeat(jnp.exp(heights), shape[position] // blocks).reshape((-1,) + (1,) * (len(shape) - position - 1))

    factor_of = one(*cuts[0])
    for cut in cuts[1:]:
        factor_of = factor_of * one(*cut)
    return factor_of


def bell_draw(own_key, extent, scale, limit, cuts=(), kind=jnp.bfloat16):
    values = scale * jax.random.normal(own_key, extent, jnp.float32)
    if cuts:
        values = values * level_of(own_key, extent, cuts, -0.22, 0.18)
    return jnp.clip(values, -limit, limit).astype(kind)


def setup_inputs(seed: int = 0) -> dict:
    arg_keys = jax.random.split(jax.random.key(seed), 12)
    signal = bell_draw(arg_keys[0], (SEQS, SEQ, D), 1.0, 6.0, ((0, 4), (1, 64)))
    gate_in = bell_draw(arg_keys[1], (SEQS, SEQ, D), 1.0, 6.0, ((0, 4), (1, 64)))
    gate_out = bell_draw(arg_keys[2], (SEQS, SEQ, D), 1.0, 6.0, ((0, 4), (1, 64)))
    pos_weight = bell_draw(arg_keys[3], (EMB, ORDER), EMB ** -0.5, 1.0, (), jnp.float32)
    pos_bias = jnp.clip(jax.random.uniform(arg_keys[4], (ORDER,), jnp.float32, -1.0, 1.0), -1.0, 1.0)
    inner_weight = bell_draw(arg_keys[5], (INNER, ORDER, ORDER), ORDER ** -0.5, 0.75, (), jnp.float32)
    inner_bias = jnp.clip(jax.random.uniform(arg_keys[6], (INNER, ORDER), jnp.float32, -1.0, 1.0), -1.0, 1.0)
    frequency = jnp.clip(jnp.exp(jax.random.uniform(arg_keys[7], (ORDER,), jnp.float32, math.log(1.0), math.log(12.0))), 1.0, 12.0)
    out_weight = bell_draw(arg_keys[8], (ORDER, D), ORDER ** -0.5, 0.75, (), jnp.float32)
    decay_rates = jnp.clip(jnp.exp(jax.random.uniform(arg_keys[9], (D,), jnp.float32, math.log(0.3), math.log(3000.0))), 0.3, 3000.0)
    skip_gain = bell_draw(arg_keys[10], (D,), 1.0, 6.0, (), jnp.float32)
    return dict(signal=signal, gate_in=gate_in, gate_out=gate_out, pos_weight=pos_weight, pos_bias=pos_bias, inner_weight=inner_weight, inner_bias=inner_bias, frequency=frequency, out_weight=out_weight, decay_rates=decay_rates, skip_gain=skip_gain)


TWO_PI = 6.283185307179586
FLOOR_SHIFT = 0.05
EPSILON = 1e-06
HIGHEST = lax.Precision.HIGHEST

def unit_angle(index, period):
    return (index % period).astype(jnp.float32) * (TWO_PI / period)

def section_tables(row_ids, col_ids, period):
    angle = unit_angle(row_ids[:, None] * col_ids[None, :], period)
    return (jnp.cos(angle).astype(jnp.bfloat16), jnp.sin(angle).astype(jnp.bfloat16))

def filter_rows(positions, total, pos_weight, pos_bias, inner_weight, inner_bias, frequency, out_weight, decay_rates):
    band_count = (pos_weight.shape[0] - 1) // 2
    position_f = positions.astype(jnp.float32)
    moments = position_f / (total - 1)
    phases = position_f * (TWO_PI / total)
    tone_list = jnp.linspace(0.0001, band_count - 1, band_count).astype(jnp.float32)
    angles = tone_list[:, None] * phases[None, :]
    features = jnp.concatenate([moments[None, :], jnp.cos(angles), -jnp.sin(angles)], axis=0)
    hidden = jnp.sin(frequency[:, None] * (jnp.dot(pos_weight.T, features, precision=HIGHEST) + pos_bias[:, None]))
    for layer_index in range(inner_weight.shape[0]):
        hidden = jnp.sin(frequency[:, None] * (jnp.dot(inner_weight[layer_index].T, hidden, precision=HIGHEST) + inner_bias[layer_index][:, None]))
    shaped = lax.dot_general(hidden, out_weight, (((0,), (0,)), ((), ())), precision=HIGHEST)
    return shaped * (jnp.exp(-moments[:, None] * decay_rates[None, :]) + FLOOR_SHIFT)

def forward_first(source, fwd_cos, fwd_sin, blocks, rows_freq):
    span = source.shape[0] // blocks
    width = source.shape[1]
    flat = source.reshape(blocks, span * width)
    real_part = jnp.dot(fwd_cos, flat, preferred_element_type=jnp.float32)
    imag_part = -jnp.dot(fwd_sin, flat, preferred_element_type=jnp.float32)
    return (real_part.astype(jnp.bfloat16).reshape(rows_freq, span, width), imag_part.astype(jnp.bfloat16).reshape(rows_freq, span, width))

def row_tables(row_id, span, rows_freq, period):
    column_ids = jnp.arange(span, dtype=jnp.int32)
    return section_tables(row_id + rows_freq * column_ids, column_ids, period)

def forward_row(cosines, sines, part_real, part_imag):
    spec_real = jnp.dot(cosines, part_real, preferred_element_type=jnp.float32) + jnp.dot(sines, part_imag, preferred_element_type=jnp.float32)
    spec_imag = jnp.dot(cosines, part_imag, preferred_element_type=jnp.float32) - jnp.dot(sines, part_real, preferred_element_type=jnp.float32)
    return (spec_real, spec_imag)

def reference(signal, gate_in, gate_out, pos_weight, pos_bias, inner_weight, inner_bias, frequency, out_weight, decay_rates, skip_gain):
    blocks = N_SEQ
    span = POS_DEV
    length = SEQ
    rows_freq = 2 * blocks
    period = 2 * length
    width = signal.shape[2]
    freq_ids = jnp.arange(rows_freq, dtype=jnp.int32)
    block_ids = jnp.arange(blocks, dtype=jnp.int32)
    shaped = filter_rows(jnp.arange(length, dtype=jnp.int32), length, pos_weight, pos_bias, inner_weight, inner_bias, frequency, out_weight, decay_rates)
    scale = lax.rsqrt(lax.optimization_barrier(jnp.sum(shaped * shaped, axis=0)) + EPSILON)
    filter_taps = shaped.astype(jnp.bfloat16)
    fwd_cos, fwd_sin = section_tables(freq_ids, block_ids, rows_freq)
    back_cos, back_sin = section_tables(block_ids, freq_ids, rows_freq)
    taps_real, taps_imag = forward_first(filter_taps, fwd_cos, fwd_sin, blocks, rows_freq)

    def filter_row(pieces):
        part_real, part_imag, row_id = pieces
        cosines, sines = row_tables(row_id, span, rows_freq, period)
        spec_real, spec_imag = forward_row(cosines, sines, part_real, part_imag)
        return (spec_real.astype(jnp.bfloat16), spec_imag.astype(jnp.bfloat16))
    filter_real, filter_imag = lax.map(filter_row, (taps_real, taps_imag, freq_ids))

    def one_sequence(pieces):
        source, gate_first, gate_second = pieces
        gated = (gate_first.astype(jnp.float32) * source.astype(jnp.float32)).astype(jnp.bfloat16)
        part_real, part_imag = forward_first(gated, fwd_cos, fwd_sin, blocks, rows_freq)

        def data_row(entries):
            row_real, row_imag, spec_real, spec_imag, row_id = entries
            cosines, sines = row_tables(row_id, span, rows_freq, period)
            wave_real, wave_imag = forward_row(cosines, sines, row_real, row_imag)
            filt_real = spec_real.astype(jnp.float32)
            filt_imag = spec_imag.astype(jnp.float32)
            prod_real = ((wave_real * filt_real - wave_imag * filt_imag) * scale).astype(jnp.bfloat16)
            prod_imag = ((wave_real * filt_imag + wave_imag * filt_real) * scale).astype(jnp.bfloat16)
            back_real = jnp.dot(cosines.T, prod_real, preferred_element_type=jnp.float32) - jnp.dot(sines.T, prod_imag, preferred_element_type=jnp.float32)
            back_imag = jnp.dot(cosines.T, prod_imag, preferred_element_type=jnp.float32) + jnp.dot(sines.T, prod_real, preferred_element_type=jnp.float32)
            return (back_real.astype(jnp.bfloat16), back_imag.astype(jnp.bfloat16))
        back_real, back_imag = lax.map(data_row, (part_real, part_imag, filter_real, filter_imag, freq_ids))
        flat_real = back_real.reshape(rows_freq, span * width)
        flat_imag = back_imag.reshape(rows_freq, span * width)
        convolved = (jnp.dot(back_cos, flat_real, preferred_element_type=jnp.float32) - jnp.dot(back_sin, flat_imag, preferred_element_type=jnp.float32)) * (1.0 / period)
        convolved = convolved.reshape(length, width)
        mixed = gate_second.astype(jnp.float32) * (convolved + skip_gain[None, :] * gated.astype(jnp.float32))
        return mixed.astype(jnp.bfloat16)
    return lax.map(one_sequence, (signal, gate_in, gate_out))
```

```python
import functools

import jax
import jax.numpy as jnp
import numpy as np
from jax import lax
from jax.experimental import pallas as pl
from jax.experimental.pallas import tpu as pltpu
from jax.sharding import PartitionSpec as P

FLOOR_SHIFT = 0.05
EPSILON = 1e-06
HIGHEST = lax.Precision.HIGHEST
F32 = jnp.float32
BF16 = jnp.bfloat16
SINE = (
    6.283182818534707,
    -41.34142139736154,
    81.5961838429123,
    -76.58010024733522,
    41.20539373944452,
    -12.271260700128162,
)


def sine_of_turns(turns):
    r = turns - jnp.round(turns)
    r2 = r * r
    poly = jnp.full_like(r2, SINE[-1])
    for factor in SINE[-2::-1]:
        poly = poly * r2 + factor
    return poly * r


def transform_tables(blocks, span):
    rows = np.arange(blocks) + 0.5
    turn = 2.0 * np.pi * np.outer(rows, np.arange(blocks)) / (2 * blocks)
    first = np.concatenate([np.cos(turn), -np.sin(turn)], axis=0)
    last = np.concatenate([np.cos(turn.T), -np.sin(turn.T)], axis=1) / (blocks * span)
    bend = 2.0 * np.pi * np.outer(rows, np.arange(span)) / (2 * blocks * span)
    twiddle = np.stack([np.cos(bend), -np.sin(bend)])
    cols = 2.0 * np.pi * (np.outer(np.arange(span), np.arange(span)) % span) / span
    cosines, sines = np.cos(cols), np.sin(cols)
    forward = np.block([[cosines, -sines], [sines, cosines]])
    backward = np.block([[cosines, sines], [-sines, cosines]])
    return (
        jnp.asarray(first, BF16),
        jnp.asarray(last, BF16),
        jnp.asarray(twiddle, F32),
        jnp.asarray(forward, BF16),
        jnp.asarray(backward, BF16),
    )


def gate_kernel(signal_ref, gate_ref, out_ref):
    gated = gate_ref[...].astype(F32) * signal_ref[...].astype(F32)
    out_ref[...] = gated.astype(BF16).T


def spectrum_of(rows_ref, group, count, blocks, channels, first, twiddle_ref, forward):
    span = rows_ref.shape[1]
    taken = [
        rows_ref[pl.ds(group * count + j, blocks, stride=channels), :].astype(BF16)
        for j in range(count)
    ]
    section = jnp.dot(first, jnp.concatenate(taken, axis=1), preferred_element_type=F32)
    cosines, sines = twiddle_ref[0], twiddle_ref[1]
    turned = []
    for j in range(count):
        real = section[:blocks, j * span : (j + 1) * span]
        imag = section[blocks:, j * span : (j + 1) * span]
        turned.append(
            jnp.concatenate(
                [
                    (real * cosines - imag * sines).astype(BF16),
                    (real * sines + imag * cosines).astype(BF16),
                ],
                axis=1,
            )
        )
    return jnp.dot(jnp.concatenate(turned, axis=0), forward, preferred_element_type=F32)


def filter_kernel(
    total,
    count,
    pos_weight_ref,
    columns_ref,
    inner_ref,
    out_weight_ref,
    decay_ref,
    first_ref,
    twiddle_ref,
    forward_ref,
    spec_ref,
    taps_ref,
    square_ref,
):
    channels = out_weight_ref.shape[0]
    span = taps_ref.shape[1]
    blocks = taps_ref.shape[0] // channels
    step_blocks = 8
    width = step_blocks * span
    layers = inner_ref.shape[0]
    bands = (pos_weight_ref.shape[1] - 1) // 2
    frequency = columns_ref[:, 0:1]
    turns_per = frequency * (1.0 / (2.0 * np.pi))
    biases = [columns_ref[:, i + 1 : i + 2] for i in range(layers + 1)]
    weight_time = pos_weight_ref[:, 0:1]
    weight_tone = pos_weight_ref[:, 1:]
    decay = decay_ref[...]
    tone = 0.0001 + lax.broadcasted_iota(jnp.int32, (bands, 1), 0).astype(F32) * (
        (bands - 1 - 0.0001) / (bands - 1)
    )
    square_ref[...] = jnp.zeros_like(square_ref)

    def positions_step(step, carry):
        position = (
            lax.broadcasted_iota(jnp.int32, (1, width), 1) + step * width
        ).astype(F32)
        moment = position / (total - 1)
        angle = tone * (position * (1.0 / total))
        features = jnp.concatenate(
            [sine_of_turns(angle + 0.25), -sine_of_turns(angle)], axis=0
        )
        pre = jnp.dot(weight_tone, features, precision=HIGHEST, preferred_element_type=F32)
        hidden = sine_of_turns(turns_per * (pre + weight_time * moment + biases[0]))
        for i in range(layers):
            pre = jnp.dot(inner_ref[i], hidden, precision=HIGHEST, preferred_element_type=F32)
            hidden = sine_of_turns(turns_per * (pre + biases[i + 1]))
        shaped = jnp.dot(
            out_weight_ref[...], hidden, precision=HIGHEST, preferred_element_type=F32
        )
        raw = shaped * (jnp.exp(-moment * decay) + FLOOR_SHIFT)
        squares = raw * raw
        folded = square_ref[...]
        for j in range(step_blocks):
            folded = folded + squares[:, j * span : (j + 1) * span]
            at = pl.multiple_of((step * step_blocks + j) * channels, channels)
            taps_ref[pl.ds(at, channels), :] = raw[:, j * span : (j + 1) * span]
        square_ref[...] = folded
        return carry

    lax.fori_loop(0, blocks // step_blocks, positions_step, 0)
    summed = jnp.sum(square_ref[...], axis=1, keepdims=True)
    square_ref[...] = jnp.broadcast_to(lax.rsqrt(summed + EPSILON), square_ref.shape)

    def spectrum_step(group, carry):
        spectrum = spectrum_of(
            taps_ref, group, count, blocks, channels, first_ref[...], twiddle_ref, forward_ref[...]
        )
        pieces = []
        for j in range(count):
            scale = square_ref[pl.ds(group * count + j, 1), :]
            scale = jnp.concatenate([scale, scale], axis=1)
            pieces.append((spectrum[j * blocks : (j + 1) * blocks] * scale).astype(BF16))
        spec_ref[group] = jnp.concatenate(pieces, axis=0)
        return carry

    lax.fori_loop(0, channels // count, spectrum_step, 0)


def convolve_kernel(
    count,
    data_ref,
    spec_ref,
    first_ref,
    last_ref,
    twiddle_ref,
    forward_ref,
    backward_ref,
    out_ref,
    rows_ref,
    result_ref,
):
    blocks, channels, span = data_ref.shape
    rows_ref[...] = data_ref[...].astype(F32).reshape(blocks * channels, span)

    def group_step(group, carry):
        spectrum = spectrum_of(
            rows_ref, group, count, blocks, channels, first_ref[...], twiddle_ref, forward_ref[...]
        )
        filt = spec_ref[group].astype(F32)
        real, imag = spectrum[:, :span], spectrum[:, span:]
        filt_real, filt_imag = filt[:, :span], filt[:, span:]
        product = jnp.concatenate(
            [
                (real * filt_real - imag * filt_imag).astype(BF16),
                (real * filt_imag + imag * filt_real).astype(BF16),
            ],
            axis=1,
        )
        back = jnp.dot(product, backward_ref[...], preferred_element_type=F32)
        cosines, sines = twiddle_ref[0], twiddle_ref[1]
        turned = []
        for j in range(count):
            real = back[j * blocks : (j + 1) * blocks, :span]
            imag = back[j * blocks : (j + 1) * blocks, span:]
            turned.append(
                jnp.concatenate(
                    [
                        (real * cosines + imag * sines).astype(BF16),
                        (imag * cosines - real * sines).astype(BF16),
                    ],
                    axis=0,
                )
            )
        convolved = jnp.dot(
            last_ref[...], jnp.concatenate(turned, axis=1), preferred_element_type=F32
        )
        for j in range(count):
            result_ref[pl.ds(group * count + j, blocks, stride=channels), :] = convolved[
                :, j * span : (j + 1) * span
            ]
        return carry

    lax.fori_loop(0, channels // count, group_step, 0)
    out_ref[...] = result_ref[...].reshape(blocks, channels, span).astype(BF16)


def mix_kernel(conv_ref, signal_ref, gate_in_ref, gate_out_ref, skip_ref, out_ref):
    gated = (gate_in_ref[...].astype(F32) * signal_ref[...].astype(F32)).astype(BF16)
    conv = conv_ref[...].T.astype(F32)
    mixed = gate_out_ref[...].astype(F32) * (conv + skip_ref[...] * gated.astype(F32))
    out_ref[...] = mixed.astype(BF16)


def per_device(
    signal,
    gate_in,
    gate_out,
    pos_weight,
    pos_bias,
    inner_weight,
    inner_bias,
    frequency,
    out_weight,
    decay_rates,
    skip_gain,
):
    blocks = lax.axis_size("seq")
    block_id = lax.axis_index("seq")
    span, width = signal.shape[1:]
    channels = width // blocks
    length = blocks * span
    signal, gate_in, gate_out = signal[0], gate_in[0], gate_out[0]
    first, last, twiddle, forward, backward = transform_tables(blocks, span)
    chunk = 512
    count = 4
    groups = channels // count

    natural = pl.BlockSpec((span, chunk), lambda i: (0, i))
    swapped = pl.BlockSpec((chunk, span), lambda i: (i, 0))
    gated = pl.pallas_call(
        gate_kernel,
        grid=(width // chunk,),
        in_specs=[natural, natural],
        out_specs=swapped,
        out_shape=jax.ShapeDtypeStruct((width, span), BF16),
        name="gate",
    )(signal, gate_in)

    arrived = lax.all_to_all(
        gated.reshape(blocks, channels, span), "seq", split_axis=0, concat_axis=0, tiled=True
    )

    own_weight = lax.dynamic_slice_in_dim(out_weight, block_id * channels, channels, axis=1).T
    own_decay = lax.dynamic_slice_in_dim(decay_rates, block_id * channels, channels, axis=0)[:, None]
    columns = jnp.concatenate([frequency[None], pos_bias[None], inner_bias], axis=0).T
    spec = pl.pallas_call(
        functools.partial(filter_kernel, length, count),
        out_shape=jax.ShapeDtypeStruct((groups, count * blocks, 2 * span), BF16),
        scratch_shapes=[
            pltpu.VMEM((blocks * channels, span), F32),
            pltpu.VMEM((channels, span), F32),
        ],
        cost_estimate=pl.CostEstimate(
            flops=20_000_000_000, bytes_accessed=2_000_000, transcendentals=2_000_000
        ),
        name="filter",
    )(
        pos_weight.T,
        columns,
        jnp.swapaxes(inner_weight, 1, 2),
        own_weight,
        own_decay,
        first,
        twiddle,
        forward,
    )

    convolved = pl.pallas_call(
        functools.partial(convolve_kernel, count),
        out_shape=jax.ShapeDtypeStruct((blocks, channels, span), BF16),
        scratch_shapes=[
            pltpu.VMEM((blocks * channels, span), F32),
            pltpu.VMEM((blocks * channels, span), F32),
        ],
        name="convolve",
    )(arrived, spec, first, last, twiddle, forward, backward)

    returned = lax.all_to_all(convolved, "seq", split_axis=0, concat_axis=0, tiled=True)
    mixed = pl.pallas_call(
        mix_kernel,
        grid=(width // chunk,),
        in_specs=[
            swapped,
            natural,
            natural,
            natural,
            pl.BlockSpec((1, chunk), lambda i: (0, i)),
        ],
        out_specs=natural,
        out_shape=jax.ShapeDtypeStruct((span, width), BF16),
        name="mix",
    )(returned.reshape(width, span), signal, gate_in, gate_out, skip_gain[None])
    return mixed[None]


def solution(mesh):
    row = P("grp", "seq", None)
    return jax.shard_map(
        per_device,
        mesh=mesh,
        in_specs=(row, row, row) + (P(),) * 8,
        out_specs=row,
        check_vma=False,
    )
```

```python
import functools

import jax
import jax.numpy as jnp
import numpy as np
from jax import lax
from jax.experimental import pallas as pl
from jax.experimental.pallas import tpu as pltpu
from jax.sharding import PartitionSpec as P

FLOOR_SHIFT = 0.05
EPSILON = 1e-06
F32 = jnp.float32
BF16 = jnp.bfloat16
STEP_BLOCKS = 4
UNROLL_POSITIONS = 2
UNROLL_GROUPS = 2
SINE = (
    6.283182818534707,
    -41.34142139736154,
    81.5961838429123,
    -76.58010024733522,
    41.20539373944452,
    -12.271260700128162,
)


def sine_of_turns(turns):
    r = turns - jnp.round(turns)
    r2 = r * r
    poly = jnp.full_like(r2, SINE[-1])
    for factor in SINE[-2::-1]:
        poly = poly * r2 + factor
    return poly * r


def transform_tables(blocks, span):
    rows = np.arange(blocks) + 0.5
    turn = 2.0 * np.pi * np.outer(rows, np.arange(blocks)) / (2 * blocks)
    first = np.concatenate([np.cos(turn), -np.sin(turn)], axis=0)
    last = np.concatenate([np.cos(turn.T), -np.sin(turn.T)], axis=1) / (blocks * span)
    bend = 2.0 * np.pi * np.outer(rows, np.arange(span)) / (2 * blocks * span)
    twiddle = np.stack([np.cos(bend), -np.sin(bend)])
    cols = 2.0 * np.pi * (np.outer(np.arange(span), np.arange(span)) % span) / span
    cosines, sines = np.cos(cols), np.sin(cols)
    forward = np.block([[cosines, -sines], [sines, cosines]])
    backward = np.block([[cosines, sines], [-sines, cosines]])
    return (
        jnp.asarray(first, BF16),
        jnp.asarray(last, BF16),
        jnp.asarray(twiddle, F32),
        jnp.asarray(forward, BF16),
        jnp.asarray(backward, BF16),
    )


def column_copies(sources, places, sems, chunk):
    width = sources[0].shape[1]
    return [
        [
            pltpu.make_async_copy(
                source.at[:, pl.ds(k * chunk, chunk)],
                place.at[:, pl.ds(k * chunk, chunk)],
                sems.at[i, k],
            )
            for i, (source, place) in enumerate(zip(sources, places))
        ]
        for k in range(width // chunk)
    ]


def gate_kernel(chunk, signal_hbm, gate_hbm, out_hbm, signal_ref, gate_ref, out_ref, sems, out_sems):
    copies = column_copies((signal_hbm, gate_hbm), (signal_ref, gate_ref), sems, chunk)
    for copy in sum(copies, []):
        copy.start()
    sent = []
    for k, pair in enumerate(copies):
        for copy in pair:
            copy.wait()
        at = pl.ds(k * chunk, chunk)
        gated = gate_ref[:, at].astype(F32) * signal_ref[:, at].astype(F32)
        out_ref[at, :] = gated.astype(BF16).T
        sent.append(pltpu.make_async_copy(out_ref.at[at, :], out_hbm.at[at, :], out_sems.at[k]))
        sent[-1].start()
    for copy in sent:
        copy.wait()


def spectrum_of(rows_ref, group, count, blocks, channels, first, twiddle_ref, forward):
    span = rows_ref.shape[1]
    taken = [
        rows_ref[pl.ds(group * count + j, blocks, stride=channels), :].astype(BF16)
        for j in range(count)
    ]
    section = jnp.dot(first, jnp.concatenate(taken, axis=1), preferred_element_type=F32)
    cosines, sines = twiddle_ref[0], twiddle_ref[1]
    turned = []
    for j in range(count):
        real = section[:blocks, j * span : (j + 1) * span]
        imag = section[blocks:, j * span : (j + 1) * span]
        turned.append(
            jnp.concatenate(
                [
                    (real * cosines - imag * sines).astype(BF16),
                    (real * sines + imag * cosines).astype(BF16),
                ],
                axis=1,
            )
        )
    return jnp.dot(jnp.concatenate(turned, axis=0), forward, preferred_element_type=F32)


def split_three(value):
    high = value.astype(BF16)
    rest = value - high.astype(F32)
    middle = rest.astype(BF16)
    low = (rest - middle.astype(F32)).astype(BF16)
    return high, middle, low


def split_weights(weight):
    high, middle, low = split_three(weight)
    return jnp.concatenate([high, middle, low, high, middle, high], axis=1)


def dot_split(weights, value):
    high, middle, low = split_three(value)
    stacked = jnp.concatenate([high, high, high, middle, middle, low], axis=0)
    return jnp.dot(weights, stacked, preferred_element_type=F32)


def filter_kernel(
    total,
    count,
    step_blocks,
    pos_weight_ref,
    pos_bias_ref,
    inner_ref,
    inner_bias_ref,
    frequency_ref,
    out_weight_hbm,
    decay_hbm,
    first_ref,
    twiddle_ref,
    forward_ref,
    spec_ref,
    taps_ref,
    square_ref,
    own_ref,
    turned_ref,
    sems,
):
    span = taps_ref.shape[1]
    channels = square_ref.shape[0]
    blocks = taps_ref.shape[0] // channels
    width = step_blocks * span
    layers, order = inner_bias_ref.shape
    bands = (pos_weight_ref.shape[0] - 1) // 2
    lanes = own_ref.shape[1]
    start = lax.axis_index("seq") * channels
    inside = pl.multiple_of(start % lanes, channels)
    outside = pl.multiple_of((start // lanes) * lanes, lanes)
    copies = [
        pltpu.make_async_copy(
            out_weight_hbm.at[:, pl.ds(outside, lanes)], own_ref.at[pl.ds(0, order), :], sems.at[0]
        ),
        pltpu.make_async_copy(
            decay_hbm.at[:, pl.ds(outside, lanes)], own_ref.at[pl.ds(order, 1), :], sems.at[1]
        ),
    ]
    own_ref[pl.ds(order, own_ref.shape[0] - order), :] = jnp.zeros(
        (own_ref.shape[0] - order, lanes), F32
    )
    for copy in copies:
        copy.start()
    turns_per = frequency_ref[...] * (1.0 / (2.0 * np.pi))
    rows = [turns_per * pos_bias_ref[...], turns_per * pos_weight_ref[0:1, :]]
    rows += [turns_per * inner_bias_ref[i : i + 1, :] for i in range(layers)]
    rows.append(jnp.zeros((8 - len(rows), order), F32))
    columns = jnp.concatenate(rows, axis=0).T
    bias, time_weight = columns[:, 0:1], columns[:, 1:2]
    biases = [columns[:, i + 2 : i + 3] for i in range(layers)]
    tone_weight = split_weights((pos_weight_ref[1:, :] * turns_per).T)
    inner = [split_weights((inner_ref[i] * turns_per).T) for i in range(layers)]
    for copy in copies:
        copy.wait()
    turned_ref[...] = own_ref[...].T
    own = turned_ref[pl.ds(inside, channels), :]
    out_weight = split_weights(own[:, :order])
    decay = own[:, order : order + 1]
    tone = 0.0001 + lax.broadcasted_iota(jnp.int32, (bands, 1), 0).astype(F32) * (
        (bands - 1 - 0.0001) / (bands - 1)
    )
    square_ref[...] = jnp.zeros_like(square_ref)

    def positions_step(step, carry):
        position = (
            lax.broadcasted_iota(jnp.int32, (1, width), 1) + step * width
        ).astype(F32)
        moment = position / (total - 1)
        angle = tone * (position * (1.0 / total))
        features = jnp.concatenate(
            [sine_of_turns(angle + 0.25), -sine_of_turns(angle)], axis=0
        )
        hidden = sine_of_turns(dot_split(tone_weight, features) + (time_weight * moment + bias))
        for i in range(layers):
            hidden = sine_of_turns(dot_split(inner[i], hidden) + biases[i])
        raw = dot_split(out_weight, hidden) * (jnp.exp(-moment * decay) + FLOOR_SHIFT)
        squares = raw * raw
        folded = square_ref[...]
        for j in range(step_blocks):
            folded = folded + squares[:, j * span : (j + 1) * span]
            at = pl.multiple_of((step * step_blocks + j) * channels, channels)
            taps_ref[pl.ds(at, channels), :] = raw[:, j * span : (j + 1) * span]
        square_ref[...] = folded
        return carry

    lax.fori_loop(0, blocks // step_blocks, positions_step, 0, unroll=UNROLL_POSITIONS)
    summed = jnp.sum(square_ref[...], axis=1, keepdims=True)
    square_ref[...] = jnp.broadcast_to(lax.rsqrt(summed + EPSILON), square_ref.shape)

    def spectrum_step(group, carry):
        spectrum = spectrum_of(
            taps_ref, group, count, blocks, channels, first_ref[...], twiddle_ref, forward_ref[...]
        )
        pieces = []
        for j in range(count):
            scale = square_ref[pl.ds(group * count + j, 1), :]
            scale = jnp.concatenate([scale, scale], axis=1)
            pieces.append((spectrum[j * blocks : (j + 1) * blocks] * scale).astype(BF16))
        spec_ref[group] = jnp.concatenate(pieces, axis=0)
        return carry

    lax.fori_loop(0, channels // count, spectrum_step, 0, unroll=UNROLL_GROUPS)


def convolve_kernel(
    count,
    data_ref,
    spec_ref,
    first_ref,
    last_ref,
    twiddle_ref,
    forward_ref,
    backward_ref,
    out_ref,
    rows_ref,
    result_ref,
):
    blocks, channels, span = data_ref.shape
    rows_ref[...] = data_ref[...].astype(F32).reshape(blocks * channels, span)

    def group_step(group, carry):
        spectrum = spectrum_of(
            rows_ref, group, count, blocks, channels, first_ref[...], twiddle_ref, forward_ref[...]
        )
        filt = spec_ref[group].astype(F32)
        real, imag = spectrum[:, :span], spectrum[:, span:]
        filt_real, filt_imag = filt[:, :span], filt[:, span:]
        product = jnp.concatenate(
            [
                (real * filt_real - imag * filt_imag).astype(BF16),
                (real * filt_imag + imag * filt_real).astype(BF16),
            ],
            axis=1,
        )
        back = jnp.dot(product, backward_ref[...], preferred_element_type=F32)
        cosines, sines = twiddle_ref[0], twiddle_ref[1]
        turned = []
        for j in range(count):
            real = back[j * blocks : (j + 1) * blocks, :span]
            imag = back[j * blocks : (j + 1) * blocks, span:]
            turned.append(
                jnp.concatenate(
                    [
                        (real * cosines + imag * sines).astype(BF16),
                        (imag * cosines - real * sines).astype(BF16),
                    ],
                    axis=0,
                )
            )
        convolved = jnp.dot(
            last_ref[...], jnp.concatenate(turned, axis=1), preferred_element_type=F32
        )
        for j in range(count):
            result_ref[pl.ds(group * count + j, blocks, stride=channels), :] = convolved[
                :, j * span : (j + 1) * span
            ]
        return carry

    lax.fori_loop(0, channels // count, group_step, 0, unroll=UNROLL_GROUPS)
    out_ref[...] = result_ref[...].reshape(blocks, channels, span).astype(BF16)


def stage_kernel(signal_ref, gate_ref, out_gate_ref, skip_ref, direct_ref, held_ref):
    gated = (gate_ref[...].astype(F32) * signal_ref[...].astype(F32)).astype(BF16)
    direct_ref[...] = skip_ref[...] * gated.astype(F32)
    held_ref[...] = out_gate_ref[...]


def mix_kernel(chunk, conv_ref, direct_ref, held_ref, out_hbm, out_ref, sems):
    width = direct_ref.shape[1]
    copies = []
    for k in range(width // chunk):
        at = pl.ds(k * chunk, chunk)
        conv = conv_ref[at, :].T.astype(F32)
        mixed = held_ref[:, at].astype(F32) * (conv + direct_ref[:, at])
        out_ref[:, at] = mixed.astype(BF16)
        copies.append(pltpu.make_async_copy(out_ref.at[:, at], out_hbm.at[:, at], sems.at[k]))
        copies[-1].start()
    for copy in copies:
        copy.wait()


def per_device(
    signal,
    gate_in,
    gate_out,
    pos_weight,
    pos_bias,
    inner_weight,
    inner_bias,
    frequency,
    out_weight,
    decay_rates,
    skip_gain,
):
    blocks = lax.axis_size("seq")
    span, width = signal.shape[1:]
    channels = width // blocks
    order = out_weight.shape[0]
    length = blocks * span
    signal, gate_in, gate_out = signal[0], gate_in[0], gate_out[0]
    first, last, twiddle, forward, backward = transform_tables(blocks, span)
    chunk = 512
    chunks = width // chunk
    count = 4
    groups = channels // count
    vmem = pl.BlockSpec(memory_space=pltpu.VMEM)
    hbm = pl.BlockSpec(memory_space=pltpu.HBM)

    def params(mebibytes):
        return pltpu.CompilerParams(vmem_limit_bytes=mebibytes * 2**20)

    gated = pl.pallas_call(
        functools.partial(gate_kernel, chunk),
        in_specs=[hbm, hbm],
        out_specs=hbm,
        out_shape=jax.ShapeDtypeStruct((width, span), BF16),
        scratch_shapes=[
            pltpu.VMEM((span, width), BF16),
            pltpu.VMEM((span, width), BF16),
            pltpu.VMEM((width, span), BF16),
            pltpu.SemaphoreType.DMA((2, chunks)),
            pltpu.SemaphoreType.DMA((chunks,)),
        ],
        compiler_params=params(60),
        name="gate",
    )(signal, gate_in)

    arrived = lax.all_to_all(
        gated.reshape(blocks, channels, span), "seq", split_axis=0, concat_axis=0, tiled=True
    )

    lanes = span
    spec = pl.pallas_call(
        functools.partial(filter_kernel, length, count, STEP_BLOCKS),
        in_specs=[vmem] * 5 + [hbm, hbm] + [vmem] * 3,
        out_specs=vmem,
        out_shape=pltpu.VMEM((groups, count * blocks, 2 * span), BF16),
        scratch_shapes=[
            pltpu.VMEM((blocks * channels, span), F32),
            pltpu.VMEM((channels, span), F32),
            pltpu.VMEM((2 * blocks, lanes), F32),
            pltpu.VMEM((lanes, 2 * blocks), F32),
            pltpu.SemaphoreType.DMA((2,)),
        ],
        cost_estimate=pl.CostEstimate(
            flops=20_000_000_000, bytes_accessed=2_000_000, transcendentals=2_000_000
        ),
        compiler_params=params(12),
        name="filter",
    )(
        pos_weight,
        pos_bias[None],
        inner_weight,
        inner_bias,
        frequency[None],
        out_weight,
        decay_rates[None],
        first,
        twiddle,
        forward,
    )

    convolved = pl.pallas_call(
        functools.partial(convolve_kernel, count),
        in_specs=[vmem] * 7,
        out_specs=vmem,
        out_shape=pltpu.VMEM((blocks, channels, span), BF16),
        scratch_shapes=[
            pltpu.VMEM((blocks * channels, span), F32),
            pltpu.VMEM((blocks * channels, span), F32),
        ],
        compiler_params=params(12),
        name="convolve",
    )(arrived, spec, first, last, twiddle, forward, backward)

    returned = lax.all_to_all(convolved, "seq", split_axis=0, concat_axis=0, tiled=True)

    signal, gate_in, gate_out, _ = lax.optimization_barrier(
        (signal, gate_in, gate_out, convolved)
    )
    direct, held = pl.pallas_call(
        stage_kernel,
        in_specs=[vmem] * 4,
        out_specs=[vmem, vmem],
        out_shape=[pltpu.VMEM((span, width), F32), pltpu.VMEM((span, width), BF16)],
        cost_estimate=pl.CostEstimate(
            flops=10_000_000_000, bytes_accessed=2_000_000, transcendentals=0
        ),
        compiler_params=params(8),
        name="stage",
    )(signal, gate_in, gate_out, skip_gain[None])

    mixed = pl.pallas_call(
        functools.partial(mix_kernel, chunk),
        in_specs=[vmem] * 3,
        out_specs=hbm,
        out_shape=jax.ShapeDtypeStruct((span, width), BF16),
        scratch_shapes=[pltpu.VMEM((span, width), BF16), pltpu.SemaphoreType.DMA((chunks,))],
        compiler_params=params(8),
        name="mix",
    )(returned.reshape(width, span), direct, held)
    return mixed[None]


def solution(mesh):
    row = P("grp", "seq", None)
    return jax.shard_map(
        per_device,
        mesh=mesh,
        in_specs=(row, row, row) + (P(),) * 8,
        out_specs=row,
        check_vma=False,
    )
```

```python
import functools

import jax
import jax.numpy as jnp
import numpy as np
from jax import lax
from jax.experimental import pallas as pl
from jax.experimental.pallas import tpu as pltpu
from jax.sharding import PartitionSpec as P

FLOOR_SHIFT = 0.05
EPSILON = 1e-06
SEQ_SHAPE = (4, 2, 8)
SHIFT = (2, 1, 4)
F32 = jnp.float32
BF16 = jnp.bfloat16
STEP_BLOCKS = 16
UNROLL_GROUPS = 2
EARLY = 1
SINE = (
    6.283182818534707,
    -41.34142139736154,
    81.5961838429123,
    -76.58010024733522,
    41.20539373944452,
    -12.271260700128162,
)


def sine_of_turns(turns):
    r = turns - jnp.round(turns)
    r2 = r * r
    poly = jnp.full_like(r2, SINE[-1])
    for factor in SINE[-2::-1]:
        poly = poly * r2 + factor
    return poly * r


def exchange_order(shape):
    at = np.indices(shape).reshape(len(shape), -1)
    moved = [(place + by) % size for place, by, size in zip(at, SHIFT, shape)]
    return np.ravel_multi_index(moved, shape)


def place_in_order(index, shape):
    place, stride = 0, 1
    for by, size in zip(SHIFT[::-1], shape[::-1]):
        place = place + stride * (((index // stride) % size + size - by) % size)
        stride *= size
    return place


def transform_tables(blocks, span):
    rows = np.arange(blocks) + 0.5
    turn = 2.0 * np.pi * np.outer(rows, np.arange(blocks)) / (2 * blocks)
    first = np.concatenate([np.cos(turn), -np.sin(turn)], axis=0)
    last = np.concatenate([np.cos(turn.T), -np.sin(turn.T)], axis=1) / (blocks * span)
    bend = 2.0 * np.pi * np.outer(rows, np.arange(span)) / (2 * blocks * span)
    twiddle = np.stack([np.cos(bend), -np.sin(bend)])
    cols = 2.0 * np.pi * (np.outer(np.arange(span), np.arange(span)) % span) / span
    cosines, sines = np.cos(cols), np.sin(cols)
    forward = np.block([[cosines, -sines], [sines, cosines]])
    backward = np.block([[cosines, sines], [-sines, cosines]])
    return (
        jnp.asarray(first, BF16),
        jnp.asarray(last, BF16),
        jnp.asarray(twiddle, F32),
        jnp.asarray(forward, BF16),
        jnp.asarray(backward, BF16),
    )


def column_copies(sources, places, sems, chunk):
    width = sources[0].shape[1]
    return [
        [
            pltpu.make_async_copy(
                source.at[:, pl.ds(k * chunk, chunk)],
                place.at[:, pl.ds(k * chunk, chunk)],
                sems.at[i, k],
            )
            for i, (source, place) in enumerate(zip(sources, places))
        ]
        for k in range(width // chunk)
    ]


def gate_kernel(chunk, signal_hbm, gate_hbm, out_hbm, signal_ref, gate_ref, out_ref, sems, out_sems):
    copies = column_copies((signal_hbm, gate_hbm), (signal_ref, gate_ref), sems, chunk)
    for copy in sum(copies, []):
        copy.start()
    sent = []
    for k, pair in enumerate(copies):
        for copy in pair:
            copy.wait()
        at = pl.ds(k * chunk, chunk)
        gated = gate_ref[:, at].astype(F32) * signal_ref[:, at].astype(F32)
        out_ref[at, :] = gated.astype(BF16).T
        sent.append(pltpu.make_async_copy(out_ref.at[at, :], out_hbm.at[at, :], out_sems.at[k]))
        sent[-1].start()
    for copy in sent:
        copy.wait()


def spectrum_of(rows_ref, group, count, blocks, channels, first, twiddle_ref, forward):
    span = rows_ref.shape[1]
    taken = [
        rows_ref[pl.ds(group * count + j, blocks, stride=channels), :].astype(BF16)
        for j in range(count)
    ]
    section = jnp.dot(first, jnp.concatenate(taken, axis=1), preferred_element_type=F32)
    cosines, sines = twiddle_ref[0], twiddle_ref[1]
    turned = []
    for j in range(count):
        real = section[:blocks, j * span : (j + 1) * span]
        imag = section[blocks:, j * span : (j + 1) * span]
        turned.append(
            jnp.concatenate(
                [
                    (real * cosines - imag * sines).astype(BF16),
                    (real * sines + imag * cosines).astype(BF16),
                ],
                axis=1,
            )
        )
    return jnp.dot(jnp.concatenate(turned, axis=0), forward, preferred_element_type=F32)


def split_three(value):
    high = value.astype(BF16)
    rest = value - high.astype(F32)
    middle = rest.astype(BF16)
    low = (rest - middle.astype(F32)).astype(BF16)
    return high, middle, low


def split_weights(weight):
    high, middle, low = split_three(weight)
    none = jnp.zeros_like(high)
    return jnp.concatenate(
        [
            jnp.concatenate([high, high, high], axis=1),
            jnp.concatenate([middle, middle, none], axis=1),
            jnp.concatenate([low, none, none], axis=1),
        ],
        axis=0,
    )


def dot_split(weights, value):
    rows = weights.shape[0] // 3
    stacked = jnp.concatenate(split_three(value), axis=0)
    parts = jnp.dot(weights, stacked, preferred_element_type=F32)
    return parts[:rows] + (parts[rows : 2 * rows] + parts[2 * rows :])


def filter_body(
    total,
    count,
    step_blocks,
    pos_weight_ref,
    pos_bias_ref,
    inner_ref,
    inner_bias_ref,
    frequency_ref,
    out_weight_hbm,
    decay_hbm,
    first_ref,
    twiddle_ref,
    forward_ref,
    spec_ref,
    taps_ref,
    square_ref,
    own_ref,
    turned_ref,
    sems,
):
    span = taps_ref.shape[1]
    channels = square_ref.shape[0]
    blocks = taps_ref.shape[0] // channels
    width = step_blocks * span
    layers, order = inner_bias_ref.shape
    bands = (pos_weight_ref.shape[0] - 1) // 2
    lanes = own_ref.shape[1]
    start = place_in_order(lax.axis_index("seq"), SEQ_SHAPE) * channels
    inside = pl.multiple_of(start % lanes, channels)
    outside = pl.multiple_of((start // lanes) * lanes, lanes)
    copies = [
        pltpu.make_async_copy(
            out_weight_hbm.at[:, pl.ds(outside, lanes)], own_ref.at[pl.ds(0, order), :], sems.at[0]
        ),
        pltpu.make_async_copy(
            decay_hbm.at[:, pl.ds(outside, lanes)], own_ref.at[pl.ds(order, 1), :], sems.at[1]
        ),
    ]
    own_ref[pl.ds(order, own_ref.shape[0] - order), :] = jnp.zeros(
        (own_ref.shape[0] - order, lanes), F32
    )
    for copy in copies:
        copy.start()
    turns_per = frequency_ref[...] * (1.0 / (2.0 * np.pi))
    rows = [turns_per * pos_bias_ref[...], turns_per * pos_weight_ref[0:1, :]]
    rows += [turns_per * inner_bias_ref[i : i + 1, :] for i in range(layers)]
    rows.append(jnp.zeros((8 - len(rows), order), F32))
    columns = jnp.concatenate(rows, axis=0).T
    bias, time_weight = columns[:, 0:1], columns[:, 1:2]
    biases = [columns[:, i + 2 : i + 3] for i in range(layers)]
    tone_weight = split_weights((pos_weight_ref[1:, :] * turns_per).T)
    inner = [split_weights((inner_ref[i] * turns_per).T) for i in range(layers)]
    for copy in copies:
        copy.wait()
    turned_ref[...] = own_ref[...].T
    own = turned_ref[pl.ds(inside, channels), :]
    out_weight = split_weights(own[:, :order])
    decay = own[:, order : order + 1]
    tone = 0.0001 + lax.broadcasted_iota(jnp.int32, (bands, 1), 0).astype(F32) * (
        (bands - 1 - 0.0001) / (bands - 1)
    )
    square_ref[...] = jnp.zeros_like(square_ref)

    def positions_step(step, carry):
        position = (
            lax.broadcasted_iota(jnp.int32, (1, width), 1) + step * width
        ).astype(F32)
        moment = position / (total - 1)
        angle = tone * (position * (1.0 / total))
        features = jnp.concatenate(
            [sine_of_turns(angle + 0.25), -sine_of_turns(angle)], axis=0
        )
        hidden = sine_of_turns(dot_split(tone_weight, features) + (time_weight * moment + bias))
        for i in range(layers):
            hidden = sine_of_turns(dot_split(inner[i], hidden) + biases[i])
        raw = dot_split(out_weight, hidden) * (jnp.exp(-moment * decay) + FLOOR_SHIFT)
        squares = raw * raw
        folded = square_ref[...]
        for j in range(step_blocks):
            folded = folded + squares[:, j * span : (j + 1) * span]
            at = pl.multiple_of((step * step_blocks + j) * channels, channels)
            taps_ref[pl.ds(at, channels), :] = raw[:, j * span : (j + 1) * span]
        square_ref[...] = folded
        return carry

    lax.fori_loop(0, blocks // step_blocks, positions_step, 0)
    summed = jnp.sum(square_ref[...], axis=1, keepdims=True)
    square_ref[...] = jnp.broadcast_to(lax.rsqrt(summed + EPSILON), square_ref.shape)

    def spectrum_step(group, carry):
        spectrum = spectrum_of(
            taps_ref, group, count, blocks, channels, first_ref[...], twiddle_ref, forward_ref[...]
        )
        pieces = []
        for j in range(count):
            scale = square_ref[pl.ds(group * count + j, 1), :]
            scale = jnp.concatenate([scale, scale], axis=1)
            pieces.append((spectrum[j * blocks : (j + 1) * blocks] * scale).astype(BF16))
        spec_ref[group] = jnp.concatenate(pieces, axis=0)
        return carry

    lax.fori_loop(0, channels // count, spectrum_step, 0, unroll=UNROLL_GROUPS)


def filter_kernel(turn, held, *args):
    scalars, refs = args[:3], args[3:]
    if held:
        refs = refs[:10] + refs[11:]

    @pl.when(lax.axis_index("grp") % 2 == turn)
    def _():
        filter_body(*scalars, *refs)


def convolve_kernel(
    count,
    data_ref,
    spec_ref,
    first_ref,
    last_ref,
    twiddle_ref,
    forward_ref,
    backward_ref,
    out_ref,
    rows_ref,
    result_ref,
):
    blocks, channels, span = data_ref.shape
    rows_ref[...] = data_ref[...].astype(F32).reshape(blocks * channels, span)

    def group_step(group, carry):
        spectrum = spectrum_of(
            rows_ref, group, count, blocks, channels, first_ref[...], twiddle_ref, forward_ref[...]
        )
        filt = spec_ref[group].astype(F32)
        real, imag = spectrum[:, :span], spectrum[:, span:]
        filt_real, filt_imag = filt[:, :span], filt[:, span:]
        product = jnp.concatenate(
            [
                (real * filt_real - imag * filt_imag).astype(BF16),
                (real * filt_imag + imag * filt_real).astype(BF16),
            ],
            axis=1,
        )
        back = jnp.dot(product, backward_ref[...], preferred_element_type=F32)
        cosines, sines = twiddle_ref[0], twiddle_ref[1]
        turned = []
        for j in range(count):
            real = back[j * blocks : (j + 1) * blocks, :span]
            imag = back[j * blocks : (j + 1) * blocks, span:]
            turned.append(
                jnp.concatenate(
                    [
                        (real * cosines + imag * sines).astype(BF16),
                        (imag * cosines - real * sines).astype(BF16),
                    ],
                    axis=0,
                )
            )
        convolved = jnp.dot(
            last_ref[...], jnp.concatenate(turned, axis=1), preferred_element_type=F32
        )
        for j in range(count):
            result_ref[pl.ds(group * count + j, blocks, stride=channels), :] = convolved[
                :, j * span : (j + 1) * span
            ]
        return carry

    lax.fori_loop(0, channels // count, group_step, 0, unroll=UNROLL_GROUPS)
    out_ref[...] = result_ref[...].reshape(blocks, channels, span).astype(BF16)


def stage_kernel(signal_ref, gate_ref, out_gate_ref, skip_ref, direct_ref, held_ref):
    gated = (gate_ref[...].astype(F32) * signal_ref[...].astype(F32)).astype(BF16)
    direct_ref[...] = skip_ref[...] * gated.astype(F32)
    held_ref[...] = out_gate_ref[...]


def mix_kernel(chunk, conv_ref, direct_ref, held_ref, out_hbm, out_ref, sems):
    width = direct_ref.shape[1]
    copies = []
    for k in range(width // chunk):
        at = pl.ds(k * chunk, chunk)
        conv = conv_ref[at, :].T.astype(F32)
        mixed = held_ref[:, at].astype(F32) * (conv + direct_ref[:, at])
        out_ref[:, at] = mixed.astype(BF16)
        copies.append(pltpu.make_async_copy(out_ref.at[:, at], out_hbm.at[:, at], sems.at[k]))
        copies[-1].start()
    for copy in copies:
        copy.wait()


def per_device(
    signal,
    gate_in,
    gate_out,
    pos_weight,
    pos_bias,
    inner_weight,
    inner_bias,
    frequency,
    out_weight,
    decay_rates,
    skip_gain,
):
    blocks = lax.axis_size("seq")
    span, width = signal.shape[1:]
    channels = width // blocks
    length = blocks * span
    signal, gate_in, gate_out = signal[0], gate_in[0], gate_out[0]
    first, last, twiddle, forward, backward = transform_tables(blocks, span)
    order = exchange_order(SEQ_SHAPE)
    first_data, last = first[:, order], last[order]
    exchange = functools.partial(
        lax.all_to_all,
        axis_name="seq",
        split_axis=0,
        concat_axis=0,
        tiled=True,
        axis_index_groups=[[int(i) for i in order]],
    )
    chunk = 512
    chunks = width // chunk
    count = 16
    groups = channels // count
    vmem = pl.BlockSpec(memory_space=pltpu.VMEM)
    hbm = pl.BlockSpec(memory_space=pltpu.HBM)

    def params(mebibytes):
        return pltpu.CompilerParams(vmem_limit_bytes=mebibytes * 2**20)

    gated = pl.pallas_call(
        functools.partial(gate_kernel, chunk),
        in_specs=[hbm, hbm],
        out_specs=hbm,
        out_shape=jax.ShapeDtypeStruct((width, span), BF16),
        scratch_shapes=[
            pltpu.VMEM((span, width), BF16),
            pltpu.VMEM((span, width), BF16),
            pltpu.VMEM((width, span), BF16),
            pltpu.SemaphoreType.DMA((2, chunks)),
            pltpu.SemaphoreType.DMA((chunks,)),
        ],
        compiler_params=params(60),
        name="gate",
    )(signal, gate_in)

    lanes = span
    shape = pltpu.VMEM((groups, count * blocks, 2 * span), BF16)

    def filter_spectrum(turn, held):
        def call(*args):
            return filter_kernel(turn, held is not None, length, count, STEP_BLOCKS, *args)

        return pl.pallas_call(
            call,
            in_specs=[vmem] * 5 + [hbm, hbm] + [vmem] * (3 if held is None else 4),
            out_specs=vmem,
            out_shape=shape,
            input_output_aliases={} if held is None else {10: 0},
            scratch_shapes=[
                pltpu.VMEM((blocks * channels, span), F32),
                pltpu.VMEM((channels, span), F32),
                pltpu.VMEM((2 * blocks, lanes), F32),
                pltpu.VMEM((lanes, 2 * blocks), F32),
                pltpu.SemaphoreType.DMA((2,)),
            ],
            cost_estimate=pl.CostEstimate(
                flops=20_000_000_000, bytes_accessed=2_000_000, transcendentals=2_000_000
            ),
            compiler_params=params(24),
            name=f"filter{turn}",
        )(
            pos_weight,
            pos_bias[None],
            inner_weight,
            inner_bias,
            frequency[None],
            out_weight,
            decay_rates[None],
            first,
            twiddle,
            forward,
            *(() if held is None else (held,)),
        )

    early = filter_spectrum(EARLY, None)
    gated, early = lax.optimization_barrier((gated, early))
    arrived = exchange(gated.reshape(blocks, channels, span))
    spec = filter_spectrum(1 - EARLY, early)

    convolved = pl.pallas_call(
        functools.partial(convolve_kernel, count),
        in_specs=[vmem] * 7,
        out_specs=vmem,
        out_shape=pltpu.VMEM((blocks, channels, span), BF16),
        scratch_shapes=[
            pltpu.VMEM((blocks * channels, span), F32),
            pltpu.VMEM((blocks * channels, span), F32),
        ],
        compiler_params=params(24),
        name="convolve",
    )(arrived, spec, first_data, last, twiddle, forward, backward)

    returned = exchange(convolved)

    signal, gate_in, gate_out, _ = lax.optimization_barrier(
        (signal, gate_in, gate_out, convolved)
    )
    direct, held = pl.pallas_call(
        stage_kernel,
        in_specs=[vmem] * 4,
        out_specs=[vmem, vmem],
        out_shape=[pltpu.VMEM((span, width), F32), pltpu.VMEM((span, width), BF16)],
        cost_estimate=pl.CostEstimate(
            flops=10_000_000_000, bytes_accessed=2_000_000, transcendentals=0
        ),
        compiler_params=params(8),
        name="stage",
    )(signal, gate_in, gate_out, skip_gain[None])

    mixed = pl.pallas_call(
        functools.partial(mix_kernel, chunk),
        in_specs=[vmem] * 3,
        out_specs=hbm,
        out_shape=jax.ShapeDtypeStruct((span, width), BF16),
        scratch_shapes=[pltpu.VMEM((span, width), BF16), pltpu.SemaphoreType.DMA((chunks,))],
        compiler_params=params(8),
        name="mix",
    )(returned.reshape(width, span), direct, held)
    return mixed[None]


def solution(mesh):
    row = P("grp", "seq", None)
    return jax.shard_map(
        per_device,
        mesh=mesh,
        in_specs=(row, row, row) + (P(),) * 8,
        out_specs=row,
        check_vma=False,
    )
```

```python
import functools

import jax
import jax.numpy as jnp
import numpy as np
from jax import lax
from jax.experimental import pallas as pl
from jax.experimental.pallas import tpu as pltpu
from jax.sharding import PartitionSpec as P

FLOOR_SHIFT = 0.05
EPSILON = 1e-06
SEQ_SHAPE = (4, 2, 8)
SHIFT = (2, 1, 4)
F32 = jnp.float32
BF16 = jnp.bfloat16
STEP_BLOCKS = 16
EARLY = 1
SINE = (
    6.283182818534707,
    -41.34142139736154,
    81.5961838429123,
    -76.58010024733522,
    41.20539373944452,
    -12.271260700128162,
)


def sine_of_turns(turns):
    r = turns - jnp.round(turns)
    r2 = r * r
    poly = jnp.full_like(r2, SINE[-1])
    for factor in SINE[-2::-1]:
        poly = poly * r2 + factor
    return poly * r


def exchange_order(shape):
    at = np.indices(shape).reshape(len(shape), -1)
    moved = [(place + by) % size for place, by, size in zip(at, SHIFT, shape)]
    return np.ravel_multi_index(moved, shape)


def place_in_order(index, shape):
    place, stride = 0, 1
    for by, size in zip(SHIFT[::-1], shape[::-1]):
        place = place + stride * (((index // stride) % size + size - by) % size)
        stride *= size
    return place


def transform_tables(blocks, span):
    rows = np.arange(blocks) + 0.5
    turn = 2.0 * np.pi * np.outer(rows, np.arange(blocks)) / (2 * blocks)
    first = np.concatenate([np.cos(turn), -np.sin(turn)], axis=0)
    last = np.concatenate([np.cos(turn.T), -np.sin(turn.T)], axis=1) / (blocks * span)
    bend = 2.0 * np.pi * np.outer(rows, np.arange(span)) / (2 * blocks * span)
    twiddle = np.stack([np.cos(bend), -np.sin(bend)])
    cols = 2.0 * np.pi * (np.outer(np.arange(span), np.arange(span)) % span) / span
    cosines, sines = np.cos(cols), np.sin(cols)
    forward = np.block([[cosines, -sines], [sines, cosines]])
    backward = np.block([[cosines, sines], [-sines, cosines]])
    return (
        jnp.asarray(first, BF16),
        jnp.asarray(last, BF16),
        jnp.asarray(twiddle, F32),
        jnp.asarray(forward, BF16),
        jnp.asarray(backward, BF16),
    )


def column_copies(sources, places, sems, chunk):
    width = sources[0].shape[1]
    return [
        [
            pltpu.make_async_copy(
                source.at[:, pl.ds(k * chunk, chunk)],
                place.at[:, pl.ds(k * chunk, chunk)],
                sems.at[i, k],
            )
            for i, (source, place) in enumerate(zip(sources, places))
        ]
        for k in range(width // chunk)
    ]


def gate_kernel(chunk, signal_hbm, gate_hbm, out_hbm, signal_ref, gate_ref, out_ref, sems, out_sems):
    copies = column_copies((signal_hbm, gate_hbm), (signal_ref, gate_ref), sems, chunk)
    for copy in sum(copies, []):
        copy.start()
    sent = []
    for k, pair in enumerate(copies):
        for copy in pair:
            copy.wait()
        at = pl.ds(k * chunk, chunk)
        gated = gate_ref[:, at].astype(F32) * signal_ref[:, at].astype(F32)
        out_ref[at, :] = gated.astype(BF16).T
        sent.append(pltpu.make_async_copy(out_ref.at[at, :], out_hbm.at[at, :], out_sems.at[k]))
        sent[-1].start()
    for copy in sent:
        copy.wait()


def spectrum_of(rows_ref, group, count, blocks, channels, first, twiddle_ref, forward):
    span = rows_ref.shape[1]
    taken = [
        rows_ref[pl.ds(group * count + j, blocks, stride=channels), :].astype(BF16)
        for j in range(count)
    ]
    section = jnp.dot(first, jnp.concatenate(taken, axis=1), preferred_element_type=F32)
    cosines, sines = twiddle_ref[0], twiddle_ref[1]
    turned = []
    for j in range(count):
        real = section[:blocks, j * span : (j + 1) * span]
        imag = section[blocks:, j * span : (j + 1) * span]
        turned.append(
            jnp.concatenate(
                [
                    (real * cosines - imag * sines).astype(BF16),
                    (real * sines + imag * cosines).astype(BF16),
                ],
                axis=1,
            )
        )
    return jnp.dot(jnp.concatenate(turned, axis=0), forward, preferred_element_type=F32)


def split_three(value):
    high = value.astype(BF16)
    rest = value - high.astype(F32)
    middle = rest.astype(BF16)
    low = (rest - middle.astype(F32)).astype(BF16)
    return high, middle, low


def split_weights(weight):
    high, middle, low = split_three(weight)
    none = jnp.zeros_like(high)
    return jnp.concatenate(
        [
            jnp.concatenate([high, high, high], axis=1),
            jnp.concatenate([middle, middle, none], axis=1),
            jnp.concatenate([low, none, none], axis=1),
        ],
        axis=0,
    )


def dot_split(weights, value):
    rows = weights.shape[0] // 3
    stacked = jnp.concatenate(split_three(value), axis=0)
    parts = jnp.dot(weights, stacked, preferred_element_type=F32)
    return parts[:rows] + (parts[rows : 2 * rows] + parts[2 * rows :])


def filter_body(
    total,
    step_blocks,
    pos_weight_ref,
    pos_bias_ref,
    inner_ref,
    inner_bias_ref,
    frequency_ref,
    out_weight_hbm,
    decay_hbm,
    taps_ref,
    square_ref,
    own_ref,
    turned_ref,
    sems,
):
    span = taps_ref.shape[1]
    channels = square_ref.shape[0]
    blocks = taps_ref.shape[0] // channels
    width = step_blocks * span
    layers, order = inner_bias_ref.shape
    bands = (pos_weight_ref.shape[0] - 1) // 2
    lanes = own_ref.shape[1]
    start = place_in_order(lax.axis_index("seq"), SEQ_SHAPE) * channels
    inside = pl.multiple_of(start % lanes, channels)
    outside = pl.multiple_of((start // lanes) * lanes, lanes)
    copies = [
        pltpu.make_async_copy(
            out_weight_hbm.at[:, pl.ds(outside, lanes)], own_ref.at[pl.ds(0, order), :], sems.at[0]
        ),
        pltpu.make_async_copy(
            decay_hbm.at[:, pl.ds(outside, lanes)], own_ref.at[pl.ds(order, 1), :], sems.at[1]
        ),
    ]
    own_ref[pl.ds(order, own_ref.shape[0] - order), :] = jnp.zeros(
        (own_ref.shape[0] - order, lanes), F32
    )
    for copy in copies:
        copy.start()
    turns_per = frequency_ref[...] * (1.0 / (2.0 * np.pi))
    rows = [turns_per * pos_bias_ref[...], turns_per * pos_weight_ref[0:1, :]]
    rows += [turns_per * inner_bias_ref[i : i + 1, :] for i in range(layers)]
    rows.append(jnp.zeros((8 - len(rows), order), F32))
    columns = jnp.concatenate(rows, axis=0).T
    bias, time_weight = columns[:, 0:1], columns[:, 1:2]
    biases = [columns[:, i + 2 : i + 3] for i in range(layers)]
    tone_weight = split_weights((pos_weight_ref[1:, :] * turns_per).T)
    inner = [split_weights((inner_ref[i] * turns_per).T) for i in range(layers)]
    for copy in copies:
        copy.wait()
    turned_ref[...] = own_ref[...].T
    own = turned_ref[pl.ds(inside, channels), :]
    out_weight = split_weights(own[:, :order])
    decay = own[:, order : order + 1]
    tone = 0.0001 + lax.broadcasted_iota(jnp.int32, (bands, 1), 0).astype(F32) * (
        (bands - 1 - 0.0001) / (bands - 1)
    )
    square_ref[...] = jnp.zeros_like(square_ref)

    def positions_step(step, carry):
        position = (
            lax.broadcasted_iota(jnp.int32, (1, width), 1) + step * width
        ).astype(F32)
        moment = position / (total - 1)
        angle = tone * (position * (1.0 / total))
        features = jnp.concatenate(
            [sine_of_turns(angle + 0.25), -sine_of_turns(angle)], axis=0
        )
        hidden = sine_of_turns(dot_split(tone_weight, features) + (time_weight * moment + bias))
        for i in range(layers):
            hidden = sine_of_turns(dot_split(inner[i], hidden) + biases[i])
        raw = dot_split(out_weight, hidden) * (jnp.exp(-moment * decay) + FLOOR_SHIFT)
        squares = raw * raw
        folded = square_ref[...]
        for j in range(step_blocks):
            folded = folded + squares[:, j * span : (j + 1) * span]
            at = pl.multiple_of((step * step_blocks + j) * channels, channels)
            taps_ref[pl.ds(at, channels), :] = raw[:, j * span : (j + 1) * span]
        square_ref[...] = folded
        return carry

    lax.fori_loop(0, blocks // step_blocks, positions_step, 0)
    summed = jnp.sum(square_ref[...], axis=1, keepdims=True)
    square_ref[...] = jnp.broadcast_to(lax.rsqrt(summed + EPSILON), square_ref.shape)


def filter_kernel(turn, total, step_blocks, *refs):
    own_turn = lax.axis_index("grp") % 2 == turn
    if len(refs) > 12:
        held_taps_ref, held_scale_ref, taps_ref, scale_ref = refs[7:11]
        refs = refs[:7] + refs[9:]

        @pl.when(jnp.logical_not(own_turn))
        def _():
            taps_ref[...] = held_taps_ref[...]
            scale_ref[...] = held_scale_ref[...]

    @pl.when(own_turn)
    def _():
        filter_body(total, step_blocks, *refs)


def spectrum_kernel(count, taps_ref, scale_ref, first_ref, twiddle_ref, forward_ref, spec_ref):
    channels = scale_ref.shape[0]
    blocks = taps_ref.shape[0] // channels
    for group in range(channels // count):
        spectrum = spectrum_of(
            taps_ref, group, count, blocks, channels, first_ref[...], twiddle_ref, forward_ref[...]
        )
        pieces = []
        for j in range(count):
            scale = scale_ref[pl.ds(group * count + j, 1), :]
            scale = jnp.concatenate([scale, scale], axis=1)
            pieces.append((spectrum[j * blocks : (j + 1) * blocks] * scale).astype(BF16))
        spec_ref[group] = jnp.concatenate(pieces, axis=0)


def convolve_kernel(
    count,
    data_ref,
    spec_ref,
    first_ref,
    last_ref,
    twiddle_ref,
    forward_ref,
    backward_ref,
    out_hbm,
    rows_ref,
    result_ref,
    out_ref,
    sems,
):
    blocks, channels, span = data_ref.shape
    rows_ref[...] = data_ref[...].astype(F32).reshape(blocks * channels, span)
    copies = []
    for group in range(channels // count):
        spectrum = spectrum_of(
            rows_ref, group, count, blocks, channels, first_ref[...], twiddle_ref, forward_ref[...]
        )
        filt = spec_ref[group].astype(F32)
        real, imag = spectrum[:, :span], spectrum[:, span:]
        filt_real, filt_imag = filt[:, :span], filt[:, span:]
        product = jnp.concatenate(
            [
                (real * filt_real - imag * filt_imag).astype(BF16),
                (real * filt_imag + imag * filt_real).astype(BF16),
            ],
            axis=1,
        )
        back = jnp.dot(product, backward_ref[...], preferred_element_type=F32)
        cosines, sines = twiddle_ref[0], twiddle_ref[1]
        turned = []
        for j in range(count):
            real = back[j * blocks : (j + 1) * blocks, :span]
            imag = back[j * blocks : (j + 1) * blocks, span:]
            turned.append(
                jnp.concatenate(
                    [
                        (real * cosines + imag * sines).astype(BF16),
                        (imag * cosines - real * sines).astype(BF16),
                    ],
                    axis=0,
                )
            )
        convolved = jnp.dot(
            last_ref[...], jnp.concatenate(turned, axis=1), preferred_element_type=F32
        )
        for j in range(count):
            result_ref[pl.ds(j, blocks, stride=count), :] = convolved[:, j * span : (j + 1) * span]
        at = pl.ds(group * count, count)
        out_ref[:, at, :] = result_ref[...].reshape(blocks, count, span).astype(BF16)
        copies.append(
            pltpu.make_async_copy(out_ref.at[:, at, :], out_hbm.at[:, at, :], sems.at[group])
        )
        copies[-1].start()
    for copy in copies:
        copy.wait()


def stage_kernel(signal_ref, gate_ref, out_gate_ref, skip_ref, direct_ref, held_ref):
    gated = (gate_ref[...].astype(F32) * signal_ref[...].astype(F32)).astype(BF16)
    direct_ref[...] = skip_ref[...] * gated.astype(F32)
    held_ref[...] = out_gate_ref[...]


def mix_kernel(chunk, conv_ref, direct_ref, held_ref, out_hbm, out_ref, sems):
    width = direct_ref.shape[1]
    copies = []
    for k in range(width // chunk):
        at = pl.ds(k * chunk, chunk)
        conv = conv_ref[at, :].T.astype(F32)
        mixed = held_ref[:, at].astype(F32) * (conv + direct_ref[:, at])
        out_ref[:, at] = mixed.astype(BF16)
        copies.append(pltpu.make_async_copy(out_ref.at[:, at], out_hbm.at[:, at], sems.at[k]))
        copies[-1].start()
    for copy in copies:
        copy.wait()


def per_device(
    signal,
    gate_in,
    gate_out,
    pos_weight,
    pos_bias,
    inner_weight,
    inner_bias,
    frequency,
    out_weight,
    decay_rates,
    skip_gain,
):
    blocks = lax.axis_size("seq")
    span, width = signal.shape[1:]
    channels = width // blocks
    length = blocks * span
    signal, gate_in, gate_out = signal[0], gate_in[0], gate_out[0]
    first, last, twiddle, forward, backward = transform_tables(blocks, span)
    order = exchange_order(SEQ_SHAPE)
    first_data, last = first[:, order], last[order]
    exchange = functools.partial(
        lax.all_to_all,
        axis_name="seq",
        split_axis=0,
        concat_axis=0,
        tiled=True,
        axis_index_groups=[[int(i) for i in order]],
    )
    chunk = 512
    chunks = width // chunk
    count = 16
    groups = channels // count
    vmem = pl.BlockSpec(memory_space=pltpu.VMEM)
    hbm = pl.BlockSpec(memory_space=pltpu.HBM)

    def params(mebibytes):
        return pltpu.CompilerParams(vmem_limit_bytes=mebibytes * 2**20)

    gated = pl.pallas_call(
        functools.partial(gate_kernel, chunk),
        in_specs=[hbm, hbm],
        out_specs=hbm,
        out_shape=jax.ShapeDtypeStruct((width, span), BF16),
        scratch_shapes=[
            pltpu.VMEM((span, width), BF16),
            pltpu.VMEM((span, width), BF16),
            pltpu.VMEM((width, span), BF16),
            pltpu.SemaphoreType.DMA((2, chunks)),
            pltpu.SemaphoreType.DMA((chunks,)),
        ],
        cost_estimate=pl.CostEstimate(
            flops=3_000_000_000, bytes_accessed=2_000_000, transcendentals=0
        ),
        compiler_params=params(60),
        name="gate",
    )(signal, gate_in)

    lanes = span
    network = (
        pos_weight,
        pos_bias[None],
        inner_weight,
        inner_bias,
        frequency[None],
        out_weight,
        decay_rates[None],
    )

    def filter_taps(turn, held):
        return pl.pallas_call(
            functools.partial(filter_kernel, turn, length, STEP_BLOCKS),
            in_specs=[vmem] * 5 + [hbm, hbm] + [vmem] * len(held),
            out_specs=[vmem] * 2,
            out_shape=[
                pltpu.VMEM((blocks * channels, span), F32),
                pltpu.VMEM((channels, span), F32),
            ],
            input_output_aliases={7: 0, 8: 1} if held else {},
            scratch_shapes=[
                pltpu.VMEM((2 * blocks, lanes), F32),
                pltpu.VMEM((lanes, 2 * blocks), F32),
                pltpu.SemaphoreType.DMA((2,)),
            ],
            cost_estimate=pl.CostEstimate(
                flops=20_000_000_000, bytes_accessed=2_000_000, transcendentals=2_000_000
            ),
            compiler_params=params(24),
            name=f"filter{turn}",
        )(*network, *held)

    taps, scale = filter_taps(EARLY, ())
    gated, scale = lax.optimization_barrier((gated, scale))
    arrived = exchange(gated.reshape(blocks, channels, span))
    taps, scale = filter_taps(1 - EARLY, (taps, scale))
    spec = pl.pallas_call(
        functools.partial(spectrum_kernel, count),
        in_specs=[vmem] * 5,
        out_specs=vmem,
        out_shape=pltpu.VMEM((groups, count * blocks, 2 * span), BF16),
        cost_estimate=pl.CostEstimate(
            flops=2_000_000_000, bytes_accessed=2_000_000, transcendentals=0
        ),
        compiler_params=params(16),
        name="spectrum",
    )(taps, scale, first, twiddle, forward)

    convolved = pl.pallas_call(
        functools.partial(convolve_kernel, count),
        in_specs=[vmem] * 7,
        out_specs=hbm,
        out_shape=jax.ShapeDtypeStruct((blocks, channels, span), BF16),
        scratch_shapes=[
            pltpu.VMEM((blocks * channels, span), F32),
            pltpu.VMEM((blocks * count, span), F32),
            pltpu.VMEM((blocks, channels, span), BF16),
            pltpu.SemaphoreType.DMA((groups,)),
        ],
        compiler_params=params(24),
        name="convolve",
    )(arrived, spec, first_data, last, twiddle, forward, backward)

    returned = exchange(convolved)

    signal, gate_in, gate_out, _ = lax.optimization_barrier(
        (signal, gate_in, gate_out, convolved)
    )
    direct, held = pl.pallas_call(
        stage_kernel,
        in_specs=[vmem] * 4,
        out_specs=[vmem, vmem],
        out_shape=[pltpu.VMEM((span, width), F32), pltpu.VMEM((span, width), BF16)],
        cost_estimate=pl.CostEstimate(
            flops=10_000_000_000, bytes_accessed=2_000_000, transcendentals=0
        ),
        compiler_params=params(8),
        name="stage",
    )(signal, gate_in, gate_out, skip_gain[None])

    mixed = pl.pallas_call(
        functools.partial(mix_kernel, chunk),
        in_specs=[vmem] * 3,
        out_specs=hbm,
        out_shape=jax.ShapeDtypeStruct((span, width), BF16),
        scratch_shapes=[pltpu.VMEM((span, width), BF16), pltpu.SemaphoreType.DMA((chunks,))],
        compiler_params=params(8),
        name="mix",
    )(returned.reshape(width, span), direct, held)
    return mixed[None]


def solution(mesh):
    row = P("grp", "seq", None)
    return jax.shard_map(
        per_device,
        mesh=mesh,
        in_specs=(row, row, row) + (P(),) * 8,
        out_specs=row,
        check_vma=False,
    )
```
